32 devices in a mesh: row: 4 (over y, core), col: 8 (over z, x).
Axes of the slice: x: 2, y: 2, z: 4, core: 2. Of those that a mesh axis runs over, the one named last changes fastest.
Arguments:
- lhat: float32 [256, 256, 256], P(('row', 'col')), may hold values from -0.375 to 0.375
- ainv_anc: float32 [256, 256, 256], P(('row', 'col')), may hold values from -2.5 to 2.5
- diag_inv: float32 [8, 256, 256], P('col', 'row'), may hold values from -0.6 to 2, as said below
- targets: int32 [256, 1], P(('row', 'col')), may hold values from 0 to 7
Outputs:
- diag_blocks: float32 [8, 256, 256], P('col', 'row')
The draws below stay inside these ranges and needn't reach their ends.
Inputs may be any that keep to these rules, and one draw needn't show every extreme that they name: `diag_inv`: each block is lower triangular with its diagonal entries between 0.5 and 2.
All inputs are finite; a program needn't handle non-finite values.
Results may differ from the reference program's by a relative error of at most 0.0003.
Values sent between devices are 32-bit elements; how exact they have to be, the bound alone decides.
A program may use at most 64 MiB of HBM per device.

```python
import jax
import jax.numpy as jnp
from jax import lax

W = 256
H = 256
SN_DEV = 1
SLOT_DEV = 8
SUPER = 8
SLOTS = 256
N_ROW = 4
N_COL = 8


def draw_diag_inv(key, part):
    first, second = jax.random.split(jax.random.fold_in(key, 17))
    spread = 0.1 * jax.random.normal(first, (SUPER, W, W), jnp.float32)
    spread = jnp.clip(spread, -0.6, 0.6)
    diagonal = jax.random.uniform(second, (SUPER, W), jnp.float32, 0.5, 2.0)
    lower = jnp.tril(spread, -1)
    return lower + diagonal[:, :, None] * jnp.eye(W, dtype=jnp.float32)[None, :, :]


def steps_of(key, extent, shards, least, high):
    factor_of = 1.0
    for dim, shards_of in shards:
        heights = jax.random.uniform(jax.random.fold_in(jax.random.fold_in(key, 6), dim), (shards_of,), jnp.float32, least / len(shards), high / len(shards))
        factor_of = factor_of * jnp.repeat(jnp.exp(heights), extent[dim] // shards_of).reshape((-1,) + (1,) * (len(extent) - 1 - dim))
    return factor_of


def picks_of(own_key, rows, number_of, top, lift):
    ranking = jax.random.permutation(jax.random.fold_in(own_key, 1), number_of)
    boost = ranking
    for power in range(3):
        boost = boost * boost // number_of
    boost = boost * lift // number_of
    tickets = jax.random.randint(jax.random.fold_in(own_key, 2), (rows, number_of), 0, 4096) + boost
    sure = jax.random.permutation(jax.random.fold_in(own_key, 3), rows)[jnp.arange(number_of) % rows]
    tickets = jnp.where(jnp.arange(rows)[:, None] == sure[None, :], 1 << 14, tickets)
    priority = tickets * number_of + jnp.arange(number_of)
    return lax.top_k(priority.astype(jnp.int32), top)[1].astype(jnp.int32)


def normal_values(stream_key, extent, width, bound, shards=(), held_as=jnp.bfloat16):
    drawn = width * jax.random.normal(stream_key, extent, jnp.float32)
    if shards:
        drawn = drawn * steps_of(stream_key, extent, shards, -0.22, 0.18)
    return jnp.clip(drawn, -bound, bound).astype(held_as)


def setup_inputs(seed: int = 0) -> dict:
    key_of = jax.random.split(jax.random.key(seed), 5)
    lhat = normal_values(key_of[0], (SLOTS, H, W), H ** -0.5, 0.375, ((0, 32),), jnp.float32)
    ainv_anc = normal_values(key_of[1], (SLOTS, H, W), ((SN_DEV / (SLOT_DEV * N_ROW)) ** 0.5), 2.5, ((0, 32),), jnp.float32)
    diag_inv = draw_diag_inv(jax.random.fold_in(key_of[4], 71), 0)
    targets = picks_of(key_of[3], SLOTS, SUPER, 1, 2048)
    return dict(lhat=lhat, ainv_anc=ainv_anc, diag_inv=diag_inv, targets=targets)


def reference(lhat, ainv_anc, diag_inv, targets):
    group_size = SLOT_DEV * N_COL
    slot_ids = targets[:, 0].reshape(N_ROW, group_size)
    left_all = lhat.reshape(N_ROW, group_size, H, W)
    right_all = ainv_anc.reshape(N_ROW, group_size, H, W)
    labels = jnp.arange(SN_DEV * N_COL, dtype=jnp.int32)

    def accumulate(running, inputs):
        left_blk, right_blk, ids_blk = inputs
        products = jnp.einsum('shi,shj->sij', left_blk, right_blk, precision=lax.Precision.HIGHEST)
        one_hot = (labels[:, None] == ids_blk[None, :]).astype(jnp.float32)
        added = jnp.einsum('ks,sij->kij', one_hot, products, precision=lax.Precision.HIGHEST)
        return running + added, None

    start_sum = jnp.zeros((SN_DEV * N_COL, W, W), jnp.float32)
    contrib, leftover = lax.scan(accumulate, start_sum, (left_all, right_all, slot_ids))
    gram_term = jnp.einsum('kia,kib->kab', diag_inv, diag_inv, precision=lax.Precision.HIGHEST)
    return gram_term - contrib
```

```python
import functools

import jax
import jax.numpy as jnp
from jax import lax
from jax.experimental import pallas as pl
from jax.experimental.pallas import tpu as pltpu
from jax.sharding import PartitionSpec as P

MESH = pl.DeviceIdType.MESH
DN = (((0,), (0,)), ((), ()))


def gram_dot(a, b):
    a_hi = a.astype(jnp.bfloat16)
    a_lo = (a - a_hi.astype(jnp.float32)).astype(jnp.bfloat16)
    b_hi = b.astype(jnp.bfloat16)
    b_lo = (b - b_hi.astype(jnp.float32)).astype(jnp.bfloat16)
    left = jnp.concatenate([a_hi, a_lo, a_hi], axis=0)
    right = jnp.concatenate([b_hi, b_hi, b_lo], axis=0)
    return lax.dot_general(left, right, DN, preferred_element_type=jnp.float32)


def kernel(
    dims,
    lhat, ainv, diag, targets, out,
    lbuf, abuf, dbuf, prod, send0, own0, recv0, send1a, send1b, recv1a, recv1b,
    sum2a, sum2b, recv2a, recv2b, sum3, recv3,
    load_sem, d_sem, s0, r0, s1a, r1a, s1b, r1b, s2a, r2a, s2b, r2b, s3, r3,
):
    yn, zn, slots, share, width = dims
    half = width // 2
    row, col = lax.axis_index("row"), lax.axis_index("col")
    y, c = lax.div(row, 2), lax.rem(row, 2)
    z, x = lax.div(col, 2), lax.rem(col, 2)

    def dev(y_, c_, z_, x_):
        return {"row": y_ * 2 + c_, "col": z_ * 2 + x_}

    shifts = [zn // 2] + [d for d in range(1, zn) if d != zn // 2] if zn > 1 else []
    order = shifts + [0]
    core_peer = dev(y, 1 - c, z, x)
    x_peer = dev(y, c, z, 1 - x)
    y_ids = [lax.rem(y + d, yn) for d in range(1, yn)]
    y_peers = [dev(i, c, z, x) for i in y_ids]
    z_peers = [dev(y, c, lax.rem(z + d, zn), x) for d in shifts]
    peers = [core_peer, x_peer] + y_peers + z_peers

    loads = []
    for s in range(slots):
        pair = (
            pltpu.make_async_copy(lhat.at[s], lbuf.at[s], load_sem.at[s, 0]),
            pltpu.make_async_copy(ainv.at[s], abuf.at[s], load_sem.at[s, 1]),
        )
        for copy in pair:
            copy.start()
        loads.append(pair)
    d_load = pltpu.make_async_copy(diag.at[0], dbuf, d_sem)
    d_load.start()

    barrier = pltpu.get_barrier_semaphore()
    for peer in peers:
        pl.semaphore_signal(barrier, inc=1, device_id=peer, device_id_type=MESH)

    for s in range(slots):
        for copy in loads[s]:
            copy.wait()
        prod[s] = gram_dot(lbuf[s], abuf[s]).reshape(yn, 2, share, width)
    d_load.wait()
    prod[slots] = gram_dot(dbuf[...], dbuf[...]).reshape(yn, 2, share, width)

    def segment(o, side, dest):
        zd = lax.rem(z + order[o], zn)
        for xi in range(2):
            k = zd * 2 + xi
            weights = [jnp.where(targets[0, s] == k, -1.0, 0.0) for s in range(slots)]
            weights.append(jnp.where(col == k, 1.0, 0.0))

            def body(yo, carry):
                for h in range(2):
                    lanes = slice(h * half, (h + 1) * half)
                    total = weights[0] * prod[0, yo, side, :, lanes]
                    for s in range(1, slots + 1):
                        total = total + weights[s] * prod[s, yo, side, :, lanes]
                    dest[o, h, xi, yo] = total
                return carry

            lax.fori_loop(0, yn, body, 0)

    def remote(src, dst, send, recv, peer):
        copy = pltpu.make_async_remote_copy(
            src_ref=src, dst_ref=dst, send_sem=send, recv_sem=recv, device_id=peer, device_id_type=MESH
        )
        copy.start()
        return copy

    started = []
    copies0, copies1a, copies1b, copies2a, copies2b = {}, {}, {}, {}, {}
    copies3 = {}

    def stage0(o):
        copies0[o] = remote(send0.at[o], recv0.at[o], s0.at[o], r0.at[o], core_peer)
        started.append(copies0[o])

    def stage1(o):
        copies0[o].wait_recv()
        send1a[o] = own0[o, 0, 1 - x] + recv0[o, 0, 1 - x]
        for i, yo in enumerate(y_ids):
            for xi in range(2):
                send1b[o, i, xi] = own0[o, 1, xi, yo] + recv0[o, 1, xi, yo]
        copies1a[o] = remote(send1a.at[o], recv1a.at[o], s1a.at[o], r1a.at[o], x_peer)
        copies1b[o] = [
            remote(send1b.at[o, i], recv1b.at[o, i], s1b.at[o, i], r1b.at[o, i], peer)
            for i, peer in enumerate(y_peers)
        ]
        started.extend([copies1a[o]] + copies1b[o])

    def stage2(o):
        copies1a[o].wait_recv()
        sum2a[o] = own0[o, 0, x] + recv0[o, 0, x] + recv1a[o]
        copies2a[o] = [
            remote(sum2a.at[o, yo], recv2a.at[o, i], s2a.at[o, i], r2a.at[o, i], peer)
            for i, (yo, peer) in enumerate(zip(y_ids, y_peers))
        ]
        for copy in copies1b[o]:
            copy.wait_recv()
        for xi in range(2):
            total = own0[o, 1, xi, y] + recv0[o, 1, xi, y]
            for i in range(yn - 1):
                total = total + recv1b[o, i, xi]
            sum2b[o, xi] = total
        copies2b[o] = remote(sum2b.at[o, 1 - x], recv2b.at[o], s2b.at[o], r2b.at[o], x_peer)
        started.extend(copies2a[o] + [copies2b[o]])

    def stage3(o):
        for copy in copies2a[o]:
            copy.wait_recv()
        total = sum2a[o, y]
        for i in range(yn - 1):
            total = total + recv2a[o, i]
        sum3[o, 0] = total
        if o < zn - 1:
            first = remote(sum3.at[o, 0], recv3.at[o, 0], s3.at[o, 0], r3.at[o, 0], z_peers[o])
        copies2b[o].wait_recv()
        sum3[o, 1] = sum2b[o, x] + recv2b[o]
        if o < zn - 1:
            second = remote(sum3.at[o, 1], recv3.at[o, 1], s3.at[o, 1], r3.at[o, 1], z_peers[o])
            copies3[o] = (first, second)
            started.extend(copies3[o])

    for o in range(zn):
        segment(o, 1 - c, send0)
        if o == 0:
            pl.semaphore_wait(barrier, len(peers))
        stage0(o)
    ahead, lag = 2, 2
    for step in range(zn + ahead + lag):
        if step < zn:
            segment(step, c, own0)
            stage1(step)
        if 0 <= step - ahead < zn:
            stage2(step - ahead)
        if 0 <= step - ahead - lag < zn:
            stage3(step - ahead - lag)

    totals = [sum3[zn - 1, h] for h in range(2)]
    for o in range(zn - 1):
        for h in range(2):
            copies3[o][h].wait_recv()
            totals[h] = totals[h] + recv3[o, h]
    for h in range(2):
        out[0, :, h * half:(h + 1) * half] = totals[h]
    for copy in started:
        copy.wait_send()


def on_device(lhat, ainv, diag, targets):
    rows, cols = lax.axis_size("row"), lax.axis_size("col")
    slots, width = lhat.shape[0], lhat.shape[2]
    height = lhat.shape[1]
    yn, zn, share = rows // 2, cols // 2, diag.shape[1]
    half = width // 2
    f32, dma = jnp.float32, pltpu.SemaphoreType.DMA
    any_space = pl.BlockSpec(memory_space=pl.ANY)
    tail = (share, half)
    scratch = [
        pltpu.VMEM((slots, height, width), f32),
        pltpu.VMEM((slots, height, width), f32),
        pltpu.VMEM((share, width), f32),
        pltpu.VMEM((slots + 1, yn, 2, share, width), f32),
        pltpu.VMEM((zn, 2, 2, yn) + tail, f32),
        pltpu.VMEM((zn, 2, 2, yn) + tail, f32),
        pltpu.VMEM((zn, 2, 2, yn) + tail, f32),
        pltpu.VMEM((zn, yn) + tail, f32),
        pltpu.VMEM((zn, yn - 1, 2) + tail, f32),
        pltpu.VMEM((zn, yn) + tail, f32),
        pltpu.VMEM((zn, yn - 1, 2) + tail, f32),
        pltpu.VMEM((zn, yn) + tail, f32),
        pltpu.VMEM((zn, 2) + tail, f32),
        pltpu.VMEM((zn, yn - 1) + tail, f32),
        pltpu.VMEM((zn,) + tail, f32),
        pltpu.VMEM((zn, 2) + tail, f32),
        pltpu.VMEM((zn - 1, 2) + tail, f32),
        dma((slots, 2)), dma,
        dma((zn,)), dma((zn,)),
        dma((zn,)), dma((zn,)),
        dma((zn, yn - 1)), dma((zn, yn - 1)),
        dma((zn, yn - 1)), dma((zn, yn - 1)),
        dma((zn,)), dma((zn,)),
        dma((zn - 1, 2)), dma((zn - 1, 2)),
    ]
    return pl.pallas_call(
        functools.partial(kernel, (yn, zn, slots, share, width)),
        out_shape=jax.ShapeDtypeStruct(diag.shape, f32),
        in_specs=[any_space, any_space, any_space, pl.BlockSpec(memory_space=pltpu.SMEM)],
        out_specs=pl.BlockSpec(memory_space=pltpu.VMEM),
        scratch_shapes=scratch,
        compiler_params=pltpu.CompilerParams(
            collective_id=0, has_side_effects=True, vmem_limit_bytes=60 * 1024 * 1024
        ),
    )(lhat, ainv, diag, targets.T)


def solution(mesh):
    placed = (
        P(("row", "col"), None, None),
        P(("row", "col"), None, None),
        P("col", "row", None),
        P(("row", "col"), None),
    )
    return jax.shard_map(
        on_device, mesh=mesh, in_specs=placed, out_specs=P("col", "row", None), check_vma=False
    )
```

```python
import functools

import jax
import jax.numpy as jnp
from jax import lax
from jax.experimental import pallas as pl
from jax.experimental.pallas import tpu as pltpu
from jax.sharding import PartitionSpec as P

MESH = pl.DeviceIdType.MESH
DN = (((0,), (0,)), ((), ()))


def gram_dot(a, b):
    a_hi = a.astype(jnp.bfloat16)
    a_lo = (a - a_hi.astype(jnp.float32)).astype(jnp.bfloat16)
    b_hi = b.astype(jnp.bfloat16)
    b_lo = (b - b_hi.astype(jnp.float32)).astype(jnp.bfloat16)
    left = jnp.concatenate([a_hi, a_lo, a_hi], axis=0)
    right = jnp.concatenate([b_hi, b_hi, b_lo], axis=0)
    return lax.dot_general(left, right, DN, preferred_element_type=jnp.float32)


def kernel(
    dims,
    lhat, ainv, diag, targets_in, out,
    targets, lbuf, abuf, dbuf, prod, send0, own0, recv0, send1a, send1b, recv1a, recv1b,
    sum2a, sum2b, recv2a, recv2b, sum3, recv3,
    load_sem, d_sem, t_sem, s0, r0, s1a, r1a, s1b, r1b, s2a, r2a, s2b, r2b, s3, r3,
):
    yn, zn, slots, share, width = dims
    half = width // 2
    row, col = lax.axis_index("row"), lax.axis_index("col")
    y, c = lax.div(row, 2), lax.rem(row, 2)
    z, x = lax.div(col, 2), lax.rem(col, 2)

    def dev(y_, c_, z_, x_):
        return {"row": y_ * 2 + c_, "col": z_ * 2 + x_}

    shifts = [zn // 2] + [d for d in range(1, zn) if d != zn // 2] if zn > 1 else []
    order = shifts + [0]
    core_peer = dev(y, 1 - c, z, x)
    x_peer = dev(y, c, z, 1 - x)
    y_ids = [lax.rem(y + d, yn) for d in range(1, yn)]
    y_peers = [dev(i, c, z, x) for i in y_ids]
    z_peers = [dev(y, c, lax.rem(z + d, zn), x) for d in shifts]
    peers = [core_peer, x_peer] + y_peers + z_peers

    t_load = pltpu.make_async_copy(targets_in, targets, t_sem)
    t_load.start()
    loads = []
    for s in range(slots):
        pair = (
            pltpu.make_async_copy(lhat.at[s], lbuf.at[s], load_sem.at[s, 0]),
            pltpu.make_async_copy(ainv.at[s], abuf.at[s], load_sem.at[s, 1]),
        )
        for copy in pair:
            copy.start()
        loads.append(pair)
    d_load = pltpu.make_async_copy(diag.at[0], dbuf, d_sem)
    d_load.start()

    barrier = pltpu.get_barrier_semaphore()
    for peer in peers:
        pl.semaphore_signal(barrier, inc=1, device_id=peer, device_id_type=MESH)

    for s in range(slots):
        for copy in loads[s]:
            copy.wait()
        prod[s] = gram_dot(lbuf[s], abuf[s]).reshape(yn, 2, share, width)
    d_load.wait()
    t_load.wait()
    prod[slots] = gram_dot(dbuf[...], dbuf[...]).reshape(yn, 2, share, width)

    def segment(o, side, dest):
        zd = lax.rem(z + order[o], zn)
        for xi in range(2):
            k = zd * 2 + xi
            weights = [jnp.where(targets[0, s] == k, -1.0, 0.0) for s in range(slots)]
            weights.append(jnp.where(col == k, 1.0, 0.0))

            def body(yo, carry):
                for h in range(2):
                    lanes = slice(h * half, (h + 1) * half)
                    total = weights[0] * prod[0, yo, side, :, lanes]
                    for s in range(1, slots + 1):
                        total = total + weights[s] * prod[s, yo, side, :, lanes]
                    dest[o, h, xi, yo] = total
                return carry

            lax.fori_loop(0, yn, body, 0)

    def remote(src, dst, send, recv, peer):
        copy = pltpu.make_async_remote_copy(
            src_ref=src, dst_ref=dst, send_sem=send, recv_sem=recv, device_id=peer, device_id_type=MESH
        )
        copy.start()
        return copy

    started = []
    copies0, copies1a, copies1b, copies2a, copies2b = {}, {}, {}, {}, {}
    copies3 = {}

    def stage0(o):
        copies0[o] = remote(send0.at[o], recv0.at[o], s0.at[o], r0.at[o], core_peer)
        started.append(copies0[o])

    def stage1(o):
        copies0[o].wait_recv()
        send1a[o] = own0[o, 0, 1 - x] + recv0[o, 0, 1 - x]
        for i, yo in enumerate(y_ids):
            for xi in range(2):
                send1b[o, i, xi] = own0[o, 1, xi, yo] + recv0[o, 1, xi, yo]
        copies1a[o] = remote(send1a.at[o], recv1a.at[o], s1a.at[o], r1a.at[o], x_peer)
        copies1b[o] = [
            remote(send1b.at[o, i], recv1b.at[o, i], s1b.at[o, i], r1b.at[o, i], peer)
            for i, peer in enumerate(y_peers)
        ]
        started.extend([copies1a[o]] + copies1b[o])

    def stage2(o):
        copies1a[o].wait_recv()
        sum2a[o] = own0[o, 0, x] + recv0[o, 0, x] + recv1a[o]
        copies2a[o] = [
            remote(sum2a.at[o, yo], recv2a.at[o, i], s2a.at[o, i], r2a.at[o, i], peer)
            for i, (yo, peer) in enumerate(zip(y_ids, y_peers))
        ]
        for copy in copies1b[o]:
            copy.wait_recv()
        for xi in range(2):
            total = own0[o, 1, xi, y] + recv0[o, 1, xi, y]
            for i in range(yn - 1):
                total = total + recv1b[o, i, xi]
            sum2b[o, xi] = total
        copies2b[o] = remote(sum2b.at[o, 1 - x], recv2b.at[o], s2b.at[o], r2b.at[o], x_peer)
        started.extend(copies2a[o] + [copies2b[o]])

    def stage3(o):
        for copy in copies2a[o]:
            copy.wait_recv()
        total = sum2a[o, y]
        for i in range(yn - 1):
            total = total + recv2a[o, i]
        sum3[o, 0] = total
        if o < zn - 1:
            first = remote(sum3.at[o, 0], recv3.at[o, 0], s3.at[o, 0], r3.at[o, 0], z_peers[o])
        copies2b[o].wait_recv()
        sum3[o, 1] = sum2b[o, x] + recv2b[o]
        if o < zn - 1:
            second = remote(sum3.at[o, 1], recv3.at[o, 1], s3.at[o, 1], r3.at[o, 1], z_peers[o])
            copies3[o] = (first, second)
            started.extend(copies3[o])

    for o in range(zn):
        segment(o, 1 - c, send0)
        if o == 0:
            pl.semaphore_wait(barrier, len(peers))
        stage0(o)
    ahead, lag = 2, 2
    for step in range(zn + ahead + lag):
        if step < zn:
            segment(step, c, own0)
            stage1(step)
        if 0 <= step - ahead < zn:
            stage2(step - ahead)
        if 0 <= step - ahead - lag < zn:
            stage3(step - ahead - lag)

    totals = [sum3[zn - 1, h] for h in range(2)]
    for o in range(zn - 1):
        for h in range(2):
            copies3[o][h].wait_recv()
            totals[h] = totals[h] + recv3[o, h]
    for h in range(2):
        out[0, :, h * half:(h + 1) * half] = totals[h]
    for copy in started:
        copy.wait_send()


def on_device(lhat, ainv, diag, targets):
    rows, cols = lax.axis_size("row"), lax.axis_size("col")
    slots, width = lhat.shape[0], lhat.shape[2]
    height = lhat.shape[1]
    yn, zn, share = rows // 2, cols // 2, diag.shape[1]
    half = width // 2
    f32, dma = jnp.float32, pltpu.SemaphoreType.DMA
    tail = (share, half)
    scratch = [
        pltpu.SMEM((1, slots), jnp.int32),
        pltpu.VMEM((slots, height, width), f32),
        pltpu.VMEM((slots, height, width), f32),
        pltpu.VMEM((share, width), f32),
        pltpu.VMEM((slots + 1, yn, 2, share, width), f32),
        pltpu.VMEM((zn, 2, 2, yn) + tail, f32),
        pltpu.VMEM((zn, 2, 2, yn) + tail, f32),
        pltpu.VMEM((zn, 2, 2, yn) + tail, f32),
        pltpu.VMEM((zn, yn) + tail, f32),
        pltpu.VMEM((zn, yn - 1, 2) + tail, f32),
        pltpu.VMEM((zn, yn) + tail, f32),
        pltpu.VMEM((zn, yn - 1, 2) + tail, f32),
        pltpu.VMEM((zn, yn) + tail, f32),
        pltpu.VMEM((zn, 2) + tail, f32),
        pltpu.VMEM((zn, yn - 1) + tail, f32),
        pltpu.VMEM((zn,) + tail, f32),
        pltpu.VMEM((zn, 2) + tail, f32),
        pltpu.VMEM((zn - 1, 2) + tail, f32),
        dma((slots, 2)), dma, dma,
        dma((zn,)), dma((zn,)),
        dma((zn,)), dma((zn,)),
        dma((zn, yn - 1)), dma((zn, yn - 1)),
        dma((zn, yn - 1)), dma((zn, yn - 1)),
        dma((zn,)), dma((zn,)),
        dma((zn - 1, 2)), dma((zn - 1, 2)),
    ]
    return pl.pallas_call(
        functools.partial(kernel, (yn, zn, slots, share, width)),
        out_shape=pltpu.VMEM(diag.shape, f32),
        in_specs=[pl.BlockSpec(memory_space=pltpu.HBM)] * 4,
        out_specs=pl.BlockSpec(memory_space=pltpu.VMEM),
        scratch_shapes=scratch,
        compiler_params=pltpu.CompilerParams(
            collective_id=0, has_side_effects=True, vmem_limit_bytes=60 * 1024 * 1024
        ),
    )(lhat, ainv, diag, targets.T)


def solution(mesh):
    placed = (
        P(("row", "col"), None, None),
        P(("row", "col"), None, None),
        P("col", "row", None),
        P(("row", "col"), None),
    )
    return jax.shard_map(
        on_device, mesh=mesh, in_specs=placed, out_specs=P("col", "row", None), check_vma=False
    )
```

```python
import functools

import jax
import jax.numpy as jnp
from jax import lax
from jax.experimental import pallas as pl
from jax.experimental.pallas import tpu as pltpu
from jax.sharding import PartitionSpec as P

MESH = pl.DeviceIdType.MESH
DN = (((0,), (0,)), ((), ()))


def gram_dot(a, b):
    a_hi = a.astype(jnp.bfloat16)
    a_lo = (a - a_hi.astype(jnp.float32)).astype(jnp.bfloat16)
    b_hi = b.astype(jnp.bfloat16)
    b_lo = (b - b_hi.astype(jnp.float32)).astype(jnp.bfloat16)
    left = jnp.concatenate([a_hi, a_lo, a_hi], axis=0)
    right = jnp.concatenate([b_hi, b_hi, b_lo], axis=0)
    return lax.dot_general(left, right, DN, preferred_element_type=jnp.float32)


def kernel(
    dims,
    lhat, ainv, diag, targets_in, out,
    targets, lbuf, abuf, dbuf, prod, send0, own0, recv0, send1a, send1b, recv1a, recv1b,
    sum2a, sum2b, recv2a, recv2b, sum3, recv3,
    load_sem, d_sem, t_sem, s0, r0, s1a, r1a, s1b, r1b, s2a, r2a, s2b, r2b, s3, r3,
):
    yn, zn, slots, share, width = dims
    half = width // 2
    row, col = lax.axis_index("row"), lax.axis_index("col")
    y, c = lax.div(row, 2), lax.rem(row, 2)
    z, x = lax.div(col, 2), lax.rem(col, 2)

    def dev(y_, c_, z_, x_):
        return {"row": y_ * 2 + c_, "col": z_ * 2 + x_}

    shifts = [zn // 2] + [d for d in range(1, zn) if d != zn // 2] if zn > 1 else []
    order = shifts + [0]
    core_peer = dev(y, 1 - c, z, x)
    x_peer = dev(y, c, z, 1 - x)
    y_ids = [lax.rem(y + d, yn) for d in range(1, yn)]
    y_peers = [dev(i, c, z, x) for i in y_ids]
    z_peers = [dev(y, c, lax.rem(z + d, zn), x) for d in shifts]
    peers = [core_peer, x_peer] + y_peers + z_peers

    t_load = pltpu.make_async_copy(targets_in, targets, t_sem)
    t_load.start()
    d_load = pltpu.make_async_copy(diag.at[0], dbuf, d_sem)
    d_load.start()
    loads = []
    for s in range(slots):
        pair = (
            pltpu.make_async_copy(lhat.at[s], lbuf.at[s], load_sem.at[s, 0]),
            pltpu.make_async_copy(ainv.at[s], abuf.at[s], load_sem.at[s, 1]),
        )
        for copy in pair:
            copy.start()
        loads.append(pair)

    barrier = pltpu.get_barrier_semaphore()
    for peer in peers:
        pl.semaphore_signal(barrier, inc=1, device_id=peer, device_id_type=MESH)

    d_load.wait()
    prod[slots] = gram_dot(dbuf[...], dbuf[...]).reshape(yn, 2, share, width)
    for s in range(slots):
        for copy in loads[s]:
            copy.wait()
        prod[s] = gram_dot(lbuf[s], abuf[s]).reshape(yn, 2, share, width)
    t_load.wait()

    def segment(o, side, dest):
        zd = lax.rem(z + order[o], zn)
        for xi in range(2):
            k = zd * 2 + xi
            weights = [jnp.where(targets[0, s] == k, -1.0, 0.0) for s in range(slots)]
            weights.append(jnp.where(col == k, 1.0, 0.0))

            def body(yo, carry):
                for h in range(2):
                    lanes = slice(h * half, (h + 1) * half)
                    total = weights[0] * prod[0, yo, side, :, lanes]
                    for s in range(1, slots + 1):
                        total = total + weights[s] * prod[s, yo, side, :, lanes]
                    dest[o, h, xi, yo] = total
                return carry

            lax.fori_loop(0, yn, body, 0, unroll=yn <= 2)

    def remote(src, dst, send, recv, peer):
        copy = pltpu.make_async_remote_copy(
            src_ref=src, dst_ref=dst, send_sem=send, recv_sem=recv, device_id=peer, device_id_type=MESH
        )
        copy.start()
        return copy

    started = []
    copies0, copies1a, copies1b, copies2a, copies2b = {}, {}, {}, {}, {}
    copies3 = {}

    def stage0(o):
        copies0[o] = remote(send0.at[o], recv0.at[o], s0.at[o], r0.at[o], core_peer)
        started.append(copies0[o])

    def stage1(o):
        copies0[o].wait_recv()
        send1a[o] = own0[o, 0, 1 - x] + recv0[o, 0, 1 - x]
        for i, yo in enumerate(y_ids):
            for xi in range(2):
                send1b[o, i, xi] = own0[o, 1, xi, yo] + recv0[o, 1, xi, yo]
        copies1a[o] = remote(send1a.at[o], recv1a.at[o], s1a.at[o], r1a.at[o], x_peer)
        copies1b[o] = [
            remote(send1b.at[o, i], recv1b.at[o, i], s1b.at[o, i], r1b.at[o, i], peer)
            for i, peer in enumerate(y_peers)
        ]
        started.extend([copies1a[o]] + copies1b[o])

    def stage2(o):
        copies1a[o].wait_recv()
        sum2a[o] = own0[o, 0, x] + recv0[o, 0, x] + recv1a[o]
        copies2a[o] = [
            remote(sum2a.at[o, yo], recv2a.at[o, i], s2a.at[o, i], r2a.at[o, i], peer)
            for i, (yo, peer) in enumerate(zip(y_ids, y_peers))
        ]
        for copy in copies1b[o]:
            copy.wait_recv()
        for xi in range(2):
            total = own0[o, 1, xi, y] + recv0[o, 1, xi, y]
            for i in range(yn - 1):
                total = total + recv1b[o, i, xi]
            sum2b[o, xi] = total
        copies2b[o] = remote(sum2b.at[o, 1 - x], recv2b.at[o], s2b.at[o], r2b.at[o], x_peer)
        started.extend(copies2a[o] + [copies2b[o]])

    def stage3(o):
        for copy in copies2a[o]:
            copy.wait_recv()
        total = sum2a[o, y]
        for i in range(yn - 1):
            total = total + recv2a[o, i]
        sum3[o, 0] = total
        if o < zn - 1:
            first = remote(sum3.at[o, 0], recv3.at[o, 0], s3.at[o, 0], r3.at[o, 0], z_peers[o])
        copies2b[o].wait_recv()
        sum3[o, 1] = sum2b[o, x] + recv2b[o]
        if o < zn - 1:
            second = remote(sum3.at[o, 1], recv3.at[o, 1], s3.at[o, 1], r3.at[o, 1], z_peers[o])
            copies3[o] = (first, second)
            started.extend(copies3[o])

    for o in range(zn):
        segment(o, 1 - c, send0)
        if o == 0:
            pl.semaphore_wait(barrier, len(peers))
        stage0(o)
    ahead, lag = 2, 2
    for step in range(zn + ahead + lag):
        if step < zn:
            segment(step, c, own0)
            stage1(step)
        if 0 <= step - ahead < zn:
            stage2(step - ahead)
        if 0 <= step - ahead - lag < zn:
            stage3(step - ahead - lag)

    totals = [sum3[zn - 1, h] for h in range(2)]
    for o in range(zn - 1):
        for h in range(2):
            copies3[o][h].wait_recv()
            totals[h] = totals[h] + recv3[o, h]
    for h in range(2):
        out[0, :, h * half:(h + 1) * half] = totals[h]
    for copy in started:
        copy.wait_send()


def on_device(lhat, ainv, diag, targets):
    rows, cols = lax.axis_size("row"), lax.axis_size("col")
    slots, width = lhat.shape[0], lhat.shape[2]
    height = lhat.shape[1]
    yn, zn, share = rows // 2, cols // 2, diag.shape[1]
    half = width // 2
    f32, dma = jnp.float32, pltpu.SemaphoreType.DMA
    tail = (share, half)
    scratch = [
        pltpu.SMEM((1, slots), jnp.int32),
        pltpu.VMEM((slots, height, width), f32),
        pltpu.VMEM((slots, height, width), f32),
        pltpu.VMEM((share, width), f32),
        pltpu.VMEM((slots + 1, yn, 2, share, width), f32),
        pltpu.VMEM((zn, 2, 2, yn) + tail, f32),
        pltpu.VMEM((zn, 2, 2, yn) + tail, f32),
        pltpu.VMEM((zn, 2, 2, yn) + tail, f32),
        pltpu.VMEM((zn, yn) + tail, f32),
        pltpu.VMEM((zn, yn - 1, 2) + tail, f32),
        pltpu.VMEM((zn, yn) + tail, f32),
        pltpu.VMEM((zn, yn - 1, 2) + tail, f32),
        pltpu.VMEM((zn, yn) + tail, f32),
        pltpu.VMEM((zn, 2) + tail, f32),
        pltpu.VMEM((zn, yn - 1) + tail, f32),
        pltpu.VMEM((zn,) + tail, f32),
        pltpu.VMEM((zn, 2) + tail, f32),
        pltpu.VMEM((zn - 1, 2) + tail, f32),
        dma((slots, 2)), dma, dma,
        dma((zn,)), dma((zn,)),
        dma((zn,)), dma((zn,)),
        dma((zn, yn - 1)), dma((zn, yn - 1)),
        dma((zn, yn - 1)), dma((zn, yn - 1)),
        dma((zn,)), dma((zn,)),
        dma((zn - 1, 2)), dma((zn - 1, 2)),
    ]
    return pl.pallas_call(
        functools.partial(kernel, (yn, zn, slots, share, width)),
        out_shape=pltpu.VMEM(diag.shape, f32),
        in_specs=[pl.BlockSpec(memory_space=pltpu.HBM)] * 4,
        out_specs=pl.BlockSpec(memory_space=pltpu.VMEM),
        scratch_shapes=scratch,
        compiler_params=pltpu.CompilerParams(
            collective_id=0, has_side_effects=True, vmem_limit_bytes=60 * 1024 * 1024
        ),
    )(lhat, ainv, diag, targets.T)


def solution(mesh):
    placed = (
        P(("row", "col"), None, None),
        P(("row", "col"), None, None),
        P("col", "row", None),
        P(("row", "col"), None),
    )
    return jax.shard_map(
        on_device, mesh=mesh, in_specs=placed, out_specs=P("col", "row", None), check_vma=False
    )
```
